256 devices in a mesh: section: 8 (over z), rep: 32 (over x, y, core).
Axes of the slice: x: 4, y: 4, z: 8, core: 2. Of those that a mesh axis runs over, the one named last changes fastest.
Arguments:
- tokens: bfloat16 [4, 4096, 1024], P(None, 'rep'), may hold values from -6 to 6
- replica_of_row: int32 [4, 4096, 1], P(None, 'rep'), may hold values from 0 to 63; in each aligned block of 128 rows (0 to 127, 128 to 255, ..., all dimensions but the last counted through in order) at most 3 rows name the same one
- widths: int32 [64], replicated, may hold values from 512 to 1024, as said below
- placement: int32 [64], replicated, may hold values from 0 to 95, as said below
- gains: float32 [8, 96, 1024], P('section', 'rep'), may hold values from 0.5 to 1.5
- weights: bfloat16 [8, 96, 1024, 1024], P('section', 'rep'), may hold values from -0.1875 to 0.1875
Outputs:
- final: bfloat16 [4, 4096, 1024], P(None, 'rep', 'section')
The draws below stay inside these ranges and needn't reach their ends.
Inputs may be any that keep to these rules, and one draw needn't show every extreme that they name: `widths`: multiples of 128 from 512 to 1024. `placement`: distinct slots; slot g lies on index g // 3 of rep. `replica_of_row`: within the 128 tokens of one index of rep in one micro-batch, no replica is named by more than 3 tokens.
All inputs are finite; a program needn't handle non-finite values.
Results may differ from the reference program's by a relative error of at most 0.008.
Values may be sent and summed in bfloat16 or wider, within the bound.
A program may use at most 64 MiB of HBM per device.

```python
import math
import jax
import jax.numpy as jnp
import numpy as np
from jax import lax

DMAX = 1024
MB = 4
ROWS = 128
REPLICAS = 64
TOTAL_SLOTS = 96
ROWS_ALL = 4096
CAP = 3
N_SECTION = 8
N_REP = 32


def draw_widths(key, part):
    units = jax.random.randint(key, (REPLICAS,), 4, 9)
    return (units * (DMAX // 8)).astype(jnp.int32)


def draw_placement(key, part):
    shuffled = jax.random.permutation(key, TOTAL_SLOTS)
    return shuffled[:REPLICAS].astype(jnp.int32)


def block_levels(rng, extent, shards, smallest, high):
    factor_of, own = 1.0, jax.random.fold_in(rng, 6)
    for axis_at, blocks in shards:
        steps = jnp.exp(jax.random.uniform(jax.random.fold_in(own, axis_at), (blocks,), jnp.float32, smallest / len(shards), high / len(shards)))
        factor_of = factor_of * jnp.repeat(steps, extent[axis_at] // blocks).reshape([-1 if axis == axis_at else 1 for axis in range(len(extent))])
    return factor_of


def assign_block(rng, own, number, rows, number_of, top, most, slope):
    order = jax.random.permutation(rng, number_of)
    crowded, usual = portions_of(number_of, rows * top, most, slope, True), portions_of(number_of, rows * top, most, slope, False)
    places = jnp.arange(number_of)

    def named(sizes, offset_by):
        used = int((sizes > 0).sum())
        fixed = max(1, used // 4)
        shifted = fixed + (places - fixed + offset_by * (used - fixed)) % max(1, number_of - fixed)
        return jnp.zeros((number_of,), jnp.int32).at[order[jnp.where(places < fixed, places, shifted)]].set(jnp.asarray(sizes, jnp.int32))

    sizes = jnp.where(number % 4 == 0, named(crowded, number // 4), named(usual, number - number // 4 - 1))
    mixed = jax.random.permutation(jax.random.fold_in(own, 3), number_of)
    source_of, receiver = mixed[0:number_of // 2 * 2:2], mixed[1:number_of // 2 * 2:2]
    room = jnp.minimum(sizes[source_of] - 1, most - sizes[receiver]) // 2
    room = jnp.where((source_of == order[0]) | (receiver == order[0]) | (sizes[receiver] == 0), 0, jnp.maximum(room, 0))
    shifted = jax.random.randint(jax.random.fold_in(own, 4), (number_of // 2,), 0, 1 << 20) % (room + 1)
    sizes = sizes.at[source_of].add(-shifted).at[receiver].add(shifted)
    items = jnp.searchsorted(jnp.cumsum(sizes), jnp.arange(rows * top), side="right").astype(jnp.int32)
    table = items.reshape(top, rows).T
    table = table[jax.random.permutation(jax.random.fold_in(own, 1), rows)]
    offset_by = jax.random.randint(jax.random.fold_in(own, 2), (rows, 1), 0, top)
    return jnp.take_along_axis(table, (jnp.arange(top)[None, :] + offset_by) % top, axis=1)


def portions_of(amount, total, most, slope, full):
    loads = [(1 << 20) // math.isqrt(grade ** slope) + 1 for grade in range(1, amount + 1)]
    largest = most if full else min(most, max(-(-total // amount), total * loads[0] // sum(loads)))
    least = 1 if total - largest >= amount - 1 else 0
    given, surplus = [largest] + [least] * (amount - 1), total - largest - least * (amount - 1)
    while surplus > 0:
        free = [i for i in range(1, amount) if given[i] < largest] or [i for i in range(1, amount) if given[i] < most]
        mass, left = sum([loads[i] for i in free]), surplus
        for i in free:
            more = min(most - given[i], max(1, left * loads[i] // mass), surplus)
            given[i] = given[i] + more
            surplus = surplus - more
    return np.array(given)


def scatter_about(stream_key, dims, spread, reach, pieces=(), kind=jnp.bfloat16):
    drawn = jax.random.normal(stream_key, dims, jnp.float32) * spread
    if len(pieces) > 0:
        drawn = block_levels(stream_key, dims, pieces, -0.22, 0.18) * drawn
    return jnp.clip(drawn, min=-reach, max=reach).astype(kind)


def setup_inputs(seed: int = 0) -> dict:
    seeds = jax.random.split(jax.random.key(seed), 7)
    tokens = scatter_about(seeds[0], (MB, ROWS_ALL, DMAX), 1.0, 6.0, ((1, 32),))
    replica_of_row_keys = jax.random.split(jax.random.fold_in(seeds[1], 1), MB * ROWS_ALL // ROWS)
    replica_of_row_turns = jax.random.permutation(jax.random.fold_in(seeds[1], 3), MB * ROWS_ALL // ROWS)
    replica_of_row = jax.vmap(lambda own, number: assign_block(jax.random.fold_in(seeds[1], 2), own, number, ROWS, REPLICAS, 1, CAP, 2))(replica_of_row_keys, replica_of_row_turns).reshape((MB, ROWS_ALL, 1))
    widths = draw_widths(jax.random.fold_in(seeds[6], 71), 0)
    placement = draw_placement(jax.random.fold_in(seeds[6], 71), 0)
    gains = jnp.clip(1.0 + 0.1 * jax.random.normal(seeds[4], (N_SECTION, TOTAL_SLOTS, DMAX), jnp.float32), 0.5, 1.5)
    weights = scatter_about(seeds[5], (N_SECTION, TOTAL_SLOTS, DMAX, DMAX), DMAX ** -0.5, 0.1875, ((0, 8), (1, 32)))
    return dict(tokens=tokens, replica_of_row=replica_of_row, widths=widths, placement=placement, gains=gains, weights=weights)


epsilon = 1e-05

def replica_layer(block, weight, gain, width):
    features = jnp.arange(block.shape[1], dtype=jnp.int32)
    is_live = (features < width).astype(jnp.float32)
    float_rows = block.astype(jnp.float32)
    mean_square = lax.optimization_barrier(jnp.sum(float_rows * float_rows, axis=1)) / width.astype(jnp.float32)
    lowered = (float_rows * lax.rsqrt(mean_square + epsilon)[:, None] * gain[None, :]).astype(jnp.bfloat16)
    projected = jnp.dot(lowered, weight, preferred_element_type=jnp.float32)
    return (float_rows + jax.nn.silu(projected) * is_live[None, :]).astype(jnp.bfloat16)

def apply_item(item):
    return replica_layer(item[0], item[1], item[2], item[3])

def reference(tokens, replica_of_row, widths, placement, gains, weights):
    batches, row_total, width_max = tokens.shape
    total = batches * row_total
    row_replica = replica_of_row.reshape(total).astype(jnp.int32)
    features = jnp.arange(width_max, dtype=jnp.int32)
    row_width = widths[row_replica]
    hidden = jnp.where(features[None, :] < row_width[:, None], tokens.reshape(total, width_max), jnp.zeros((), jnp.bfloat16))
    replica_ids = jnp.arange(REPLICAS, dtype=jnp.int32)
    counts = lax.optimization_barrier(jnp.sum((row_replica[None, :] == replica_ids[:, None]).astype(jnp.int32), axis=1))
    order = jnp.argsort(row_replica, stable=True).astype(jnp.int32)
    starts = jnp.cumsum(counts).astype(jnp.int32) - counts
    bound = batches * N_REP * CAP
    offsets = jnp.arange(bound, dtype=jnp.int32)
    position = jnp.clip(starts[:, None] + offsets[None, :], 0, total - 1).astype(jnp.int32)
    gather_index = jnp.where(offsets[None, :] < counts[:, None], order[position], total).astype(jnp.int32)
    for layer in range(N_SECTION):
        padded = jnp.concatenate([hidden, jnp.zeros((1, width_max), jnp.bfloat16)], axis=0)
        grouped = padded[gather_index]
        layer_weights = weights[layer][placement]
        layer_gains = gains[layer][placement]
        updated = lax.map(apply_item, (grouped, layer_weights, layer_gains, widths))
        hidden = hidden.at[gather_index.reshape(-1)].set(updated.reshape(-1, width_max), mode='drop')
    return hidden.reshape(batches, row_total, width_max)
```

```python
import functools

import jax
import jax.numpy as jnp
from jax import lax
from jax.experimental import pallas as pl
from jax.experimental.pallas import tpu as pltpu
from jax.sharding import PartitionSpec as P

MESH = pl.DeviceIdType.MESH
epsilon = 1e-05
LANES = 128
CHUNK = 32
GROUPS = 6


def relay_kernel(
    n,
    slots,
    x_ref,
    w_ref,
    gain_ref,
    live_ref,
    scale_ref,
    out_ref,
    land,
    done,
    weights,
    final,
    w_sem,
    gather_send,
    gather_recv,
    relay_send,
    relay_recv,
    final_send,
    final_recv,
):
    me = lax.axis_index("section")
    last = n - 1
    rows = x_ref.shape[0]
    chunks = rows // CHUNK
    per_slot = chunks // slots
    span = rows // GROUPS
    per_group = chunks // GROUPS

    for s in range(slots):
        pltpu.make_async_copy(w_ref.at[s], weights.at[s], w_sem.at[s]).start()

    barrier = pltpu.get_barrier_semaphore()
    for k in range(1, n):
        pl.semaphore_signal(
            barrier, inc=1, device_id={"section": lax.rem(me + k, n)}, device_id_type=MESH
        )
    pl.semaphore_wait(barrier, n - 1)

    my_columns = pl.ds(pl.multiple_of(me * LANES, LANES), LANES)

    @pl.when(me != 0)
    def _():
        for g in range(GROUPS):
            part = pl.ds(g * span, span)
            pltpu.make_async_remote_copy(
                src_ref=x_ref.at[part],
                dst_ref=land.at[part, my_columns],
                send_sem=gather_send,
                recv_sem=gather_recv.at[g],
                device_id={"section": 0},
                device_id_type=MESH,
            ).start()

    @pl.when(me == 0)
    def _():
        land[:, :LANES] = x_ref[...]

    def here(c):
        return pl.ds(pl.multiple_of(c * CHUNK, CHUNK), CHUNK)

    def forward(c):
        return pltpu.make_async_remote_copy(
            src_ref=done.at[here(c)],
            dst_ref=land.at[here(c)],
            send_sem=relay_send.at[c],
            recv_sem=relay_recv.at[c],
            device_id={"section": lax.rem(me + 1, n)},
            device_id_type=MESH,
        )

    def spread(c, section):
        columns = pl.ds(section * LANES, LANES)
        return pltpu.make_async_remote_copy(
            src_ref=done.at[here(c), columns],
            dst_ref=final.at[here(c)],
            send_sem=final_send.at[c],
            recv_sem=final_recv.at[c],
            device_id={"section": section},
            device_id_type=MESH,
        )

    def step(c, carry):
        @pl.when((me == 0) & (lax.rem(c, per_group) == 0))
        def _():
            g = c // per_group
            part = pl.ds(pl.multiple_of(g * span, span), span)
            others = land.at[part, LANES:]
            pltpu.make_async_copy(others, others, gather_recv.at[g]).wait()

        @pl.when(me != 0)
        def _():
            forward(c).wait_recv()

        slot = c // per_slot

        @pl.when(lax.rem(c, per_slot) == 0)
        def _():
            pltpu.make_async_copy(w_ref.at[slot], weights.at[slot], w_sem.at[slot]).wait()

        hidden = land[here(c), :].astype(jnp.float32)
        mean_square = jnp.sum(hidden * hidden, axis=1, keepdims=True) * scale_ref[slot][:, :1]
        lowered = (hidden * lax.rsqrt(mean_square + epsilon) * gain_ref[slot]).astype(jnp.bfloat16)
        projected = jnp.dot(lowered, weights[slot], preferred_element_type=jnp.float32)
        done[here(c), :] = (
            hidden + projected / (1.0 + jnp.exp(-projected)) * live_ref[slot]
        ).astype(jnp.bfloat16)

        @pl.when(me != last)
        def _():
            forward(c).start()

        @pl.when(me == last)
        def _():
            for section in range(n - 1):
                spread(c, section).start()

        return carry

    lax.fori_loop(0, chunks, step, 0)

    @pl.when(me == last)
    def _():
        out_ref[...] = done[:, last * LANES :]

        def settle(c, carry):
            sent = done.at[here(c), LANES:]
            pltpu.make_async_copy(sent, sent, final_send.at[c]).wait()
            return carry

        lax.fori_loop(0, chunks, settle, 0)

    @pl.when(me != last)
    def _():
        def settle(c, carry):
            forward(c).wait_send()
            spread(c, 0).wait_recv()
            return carry

        lax.fori_loop(0, chunks, settle, 0)
        out_ref[...] = final[...]

    @pl.when(me != 0)
    def _():
        pltpu.make_async_copy(x_ref, x_ref, gather_send).wait()


def on_device(tokens, replica_of_row, widths, placement, gains, weights):
    batches, row_count, width_max = tokens.shape
    n = lax.axis_size("section")
    rep_count = lax.axis_size("rep")
    slots = weights.shape[1]
    section_id = lax.axis_index("section")
    rep_id = lax.axis_index("rep")
    tokens_all = batches * row_count
    capacity = 3
    per_pair = slots * batches * capacity
    rows = rep_count * per_pair

    row_replica = replica_of_row[:, :, 0]
    picked = row_replica[:, :, None] == jnp.arange(widths.shape[0], dtype=jnp.int32)
    slot_of_row = jnp.sum(jnp.where(picked, placement, 0), axis=2)
    row_width = jnp.sum(jnp.where(picked, widths, 0), axis=2)
    numbers = jnp.arange(row_count, dtype=jnp.int32)
    same = (row_replica[:, :, None] == row_replica[:, None, :]) & (
        numbers[None, :] < numbers[:, None]
    )
    position = jnp.sum(same.astype(jnp.int32), axis=2)
    batch = jnp.arange(batches, dtype=jnp.int32)[:, None]
    target = (slot_of_row * (batches * capacity) + batch * capacity + position).reshape(tokens_all)

    mine = lax.dynamic_slice_in_dim(tokens, section_id * LANES, LANES, axis=2)
    features = section_id * LANES + jnp.arange(LANES, dtype=jnp.int32)
    entering = jnp.where(
        features < row_width[:, :, None], mine, jnp.zeros((), jnp.bfloat16)
    ).reshape(tokens_all, LANES)
    table = (jnp.arange(rows, dtype=jnp.int32)[:, None] == target[None, :]).astype(jnp.bfloat16)
    outgoing = jnp.dot(table, entering, preferred_element_type=jnp.float32).astype(jnp.bfloat16)
    arrived = lax.all_to_all(
        outgoing.reshape(rep_count, per_pair, LANES), "rep", 0, 0, tiled=True
    )
    dense = arrived.reshape(rep_count, slots, batches * capacity, LANES)
    dense = jnp.swapaxes(dense, 0, 1).reshape(rows, LANES)

    slot_ids = rep_id * slots + jnp.arange(slots, dtype=jnp.int32)
    slot_width = jnp.sum(jnp.where(placement[None, :] == slot_ids[:, None], widths, 0), axis=1)
    live = (jnp.arange(width_max, dtype=jnp.int32) < slot_width[:, None]).astype(jnp.float32)
    scale = 1.0 / jnp.maximum(slot_width, 1).astype(jnp.float32)
    scale = jnp.broadcast_to(scale[:, None, None], (slots, 1, LANES))

    chunks = rows // CHUNK
    vmem = pl.BlockSpec(memory_space=pltpu.VMEM)
    result = pl.pallas_call(
        functools.partial(relay_kernel, n, slots),
        out_shape=jax.ShapeDtypeStruct((rows, LANES), jnp.bfloat16),
        in_specs=[vmem, pl.BlockSpec(memory_space=pl.ANY), vmem, vmem, vmem],
        out_specs=vmem,
        scratch_shapes=[
            pltpu.VMEM((rows, width_max), jnp.bfloat16),
            pltpu.VMEM((rows, width_max), jnp.bfloat16),
            pltpu.VMEM((slots, width_max, width_max), jnp.bfloat16),
            pltpu.VMEM((rows, LANES), jnp.bfloat16),
            pltpu.SemaphoreType.DMA((slots,)),
            pltpu.SemaphoreType.DMA,
            pltpu.SemaphoreType.DMA((GROUPS,)),
            pltpu.SemaphoreType.DMA((chunks,)),
            pltpu.SemaphoreType.DMA((chunks,)),
            pltpu.SemaphoreType.DMA((chunks,)),
            pltpu.SemaphoreType.DMA((chunks,)),
        ],
        compiler_params=pltpu.CompilerParams(
            collective_id=0, has_side_effects=True, vmem_limit_bytes=40 * 1024 * 1024
        ),
        name="relay",
    )(dense, weights[0], gains[0][:, None, :], live[:, None, :], scale)

    back = jnp.swapaxes(result.reshape(slots, rep_count, batches * capacity, LANES), 0, 1)
    back = lax.all_to_all(
        back.reshape(rep_count, per_pair, LANES), "rep", 0, 0, tiled=True
    ).reshape(rows, LANES)
    final = lax.dot_general(
        table, back, (((0,), (0,)), ((), ())), preferred_element_type=jnp.float32
    ).astype(jnp.bfloat16)
    return final.reshape(batches, row_count, LANES)


def solution(mesh):
    in_specs = (
        P(None, "rep", None),
        P(None, "rep", None),
        P(),
        P(),
        P("section", "rep", None),
        P("section", "rep", None, None),
    )
    return jax.shard_map(
        on_device,
        mesh=mesh,
        in_specs=in_specs,
        out_specs=P(None, "rep", "section"),
        check_vma=False,
    )
```
